32 devices in a mesh: gx: 16 (over z, y, x), gz: 2 (over core).
Axes of the slice: x: 2, y: 2, z: 4, core: 2. Of those that a mesh axis runs over, the one named last changes fastest.
Arguments:
- velocity: float32 [3, 256, 16, 256], P(None, 'gx', 'gz'), may hold values from -6 to 6
- pressure: float32 [256, 16, 256], P('gx', 'gz'), may hold values from 1 to 3
- stress_old: float32 [6, 256, 16, 256], P(None, 'gx', 'gz'), may hold values from -6 to 6
- plastic: float32 [256, 16, 256], P('gx', 'gz'), may hold values from 0 to 2
- viscosity: float32 [256, 16, 256], P('gx', 'gz'), may hold values from 1 to 30
- weak_seed: int32 [256, 16, 256], P('gx', 'gz'), may hold values 0 or 1
Outputs:
- velocity_out: float32 [3, 256, 16, 256], P(None, 'gx', 'gz')
- pressure_out: float32 [256, 16, 256], P('gx', 'gz')
- stress_out: float32 [6, 256, 16, 256], P(None, 'gx', 'gz')
- plastic_out: float32 [256, 16, 256], P('gx', 'gz')
- yield_peak: float32 [2], replicated
The draws below stay inside these ranges and needn't reach their ends.
All inputs are finite; a program needn't handle non-finite values. No bound on the sum of `weak_seed` on one device may be relied on, other than what follows from the above.
Results may differ from the reference program's by a relative error of at most 0.000059.
Values sent between devices are 32-bit elements; how exact they have to be, the bound alone decides.
A program may use at most 64 MiB of HBM per device.

```python
import math
import jax
import jax.numpy as jnp
from jax import lax

NY = 256
ITERS = 2
NX = 256
NZ = 16


def draw_viscosity(key, part):
    xpos = jnp.arange(NX, dtype=jnp.float32) / max(NX - 1, 1)
    ramp = jnp.exp(jnp.log(10.0) * xpos)[:, None, None]
    rough = jnp.exp(jax.random.uniform(key, (NX, NZ, NY), jnp.float32, 0.0, jnp.log(3.0)))
    return (ramp * rough).astype(jnp.float32)


def touch_ends(array, rng, least, largest):
    longest = array.shape.index(max(array.shape))
    spots = []
    for shift in (0, 1):
        where = [jax.random.randint(jax.random.fold_in(rng, axis), (), 0, length) for axis, length in enumerate(array.shape)]
        where[longest] = (where[longest] + shift) % array.shape[longest]
        spots.append(tuple(where))
    return array.at[spots[0]].set(least).at[spots[1]].set(largest)


def level_of(own_key, extent, cuts, smallest, high):
    factor_of, own = 1.0, jax.random.fold_in(own_key, 6)
    for position, shards_of in cuts:
        draws = jnp.exp(jax.random.uniform(jax.random.fold_in(own, position), (shards_of,), jnp.float32, smallest / len(cuts), high / len(cuts)))
        factor_of = factor_of * jnp.repeat(draws, extent[position] // shards_of).reshape([-1 if axis == position else 1 for axis in range(len(extent))])
    return factor_of


def bell_draw(own_key, extent, deviation, limit, cuts=(), held_as=jnp.bfloat16):
    result = deviation * jax.random.normal(own_key, extent, jnp.float32)
    if cuts:
        result = result * level_of(own_key, extent, cuts, -0.22, 0.18)
    return jnp.clip(result, -limit, limit).astype(held_as)


def setup_inputs(seed: int = 0) -> dict:
    key_of = jax.random.split(jax.random.key(seed), 7)
    velocity = bell_draw(key_of[0], (3, NX, NZ, NY), 1.0, 6.0, ((1, 16), (2, 2)), jnp.float32)
    pressure = jnp.clip(1.0 + 2.0 * jax.random.uniform(key_of[1], (NX, NZ, NY), jnp.float32) ** level_of(key_of[1], (NX, NZ, NY), ((0, 16), (1, 2)), -0.2, 0.2), 1.0, 3.0)
    stress_old = bell_draw(key_of[2], (6, NX, NZ, NY), 1.0, 6.0, ((1, 16), (2, 2)), jnp.float32)
    plastic = jnp.clip(2.0 * jax.random.uniform(key_of[3], (NX, NZ, NY), jnp.float32) ** level_of(key_of[3], (NX, NZ, NY), ((0, 16), (1, 2)), -0.2, 0.2), 0.0, 2.0)
    viscosity = draw_viscosity(jax.random.fold_in(key_of[6], 71), 0)
    weak_seed = touch_ends((jax.random.randint(key_of[5], (NX, NZ, NY), 0, 8) < 1).astype(jnp.int32), jax.random.fold_in(key_of[5], 1), 0, 1)
    return {"velocity": velocity, "pressure": pressure, "stress_old": stress_old, "plastic": plastic, "viscosity": viscosity, "weak_seed": weak_seed}


unnormalized_weights = [math.exp(-(k * k) / 18.0) for k in range(-6, 7)]
weight_total = sum(unnormalized_weights)
gauss_weights = [value / weight_total for value in unnormalized_weights]
shear_time_increment = 20.0

def smooth_axis(field, axis):
    count = field.shape[axis]
    widths = [(0, 0)] * field.ndim
    widths[axis] = (6, 6)
    padded = jnp.pad(field, widths)
    total = gauss_weights[0] * lax.slice_in_dim(padded, 0, count, axis=axis)
    for index in range(1, 13):
        total = total + gauss_weights[index] * lax.slice_in_dim(padded, index, index + count, axis=axis)
    return total

def y_matrix(length):
    places = jnp.arange(length)
    gap = (places[:, None] - places[None, :]).astype(jnp.float32)
    return jnp.where(jnp.abs(gap) <= 6.0, jnp.exp(-gap * gap / 18.0) / weight_total, 0.0).astype(jnp.float32)

def smooth_y(field):
    length = field.shape[-1]
    flat = field.reshape(-1, length)
    return jnp.dot(flat, y_matrix(length), precision=lax.Precision.HIGHEST).reshape(field.shape)

def diff_axis(field, axis):
    count = field.shape[axis]
    widths = [(0, 0)] * field.ndim
    widths[axis] = (1, 1)
    padded = jnp.pad(field, widths)
    return (lax.slice_in_dim(padded, 2, count + 2, axis=axis) - lax.slice_in_dim(padded, 0, count, axis=axis)) * 0.5

def return_map(velocity_x_spacing, velocity_z_spacing, dyv, stress_old, eta_ve, pres, cohesion_strength):
    divv = velocity_x_spacing[0] + velocity_z_spacing[1] + dyv[2]
    pres = pres - 0.25 * divv
    strain = jnp.stack([velocity_x_spacing[0] - divv / 3.0, velocity_z_spacing[1] - divv / 3.0, dyv[2] - divv / 3.0, 0.5 * (velocity_x_spacing[1] + velocity_z_spacing[0]), 0.5 * (velocity_x_spacing[2] + dyv[0]), 0.5 * (velocity_z_spacing[2] + dyv[1])])
    trial = 2.0 * eta_ve * (strain + stress_old / (2.0 * shear_time_increment))
    tau_ii = jnp.sqrt(0.5 * (trial[0] ** 2 + trial[1] ** 2 + trial[2] ** 2) + trial[3] ** 2 + trial[4] ** 2 + trial[5] ** 2)
    yield_f = tau_ii - 0.5 * jnp.maximum(pres, 0.0) - 0.8660254 * cohesion_strength
    dlam = jnp.maximum(yield_f, 0.0) / (eta_ve + 0.5)
    shrink = 1.0 - eta_ve * dlam / jnp.maximum(tau_ii, 0.5)
    return (pres, trial * shrink, shrink, yield_f, dlam)

def reference(velocity, pressure, stress_old, plastic, viscosity, weak_seed):
    smoothed = smooth_y(smooth_axis(smooth_axis(plastic, 0), 1))
    eta_ve = 1.0 / (1.0 / viscosity + 1.0 / shear_time_increment)
    seeded = weak_seed.astype(jnp.float32)
    cohesion_strength = (1.0 - 0.6 * seeded) / (1.0 + 2.0 * smoothed)
    pres = pressure
    plastic_sum = plastic
    peaks = []
    tau = stress_old
    for step_index in range(ITERS):
        velocity_x_spacing = diff_axis(velocity, 1)
        velocity_z_spacing = diff_axis(velocity, 2)
        dyv = diff_axis(velocity, 3)
        pres, tau, shrink, yield_f, dlam = return_map(velocity_x_spacing, velocity_z_spacing, dyv, stress_old, eta_ve, pres, cohesion_strength)
        plastic_sum = plastic_sum + dlam
        peaks.append(jnp.max(yield_f))
        step = 0.125 / jnp.max(eta_ve * shrink)
        sxx = tau[0] - pres
        szz = tau[1] - pres
        syy = tau[2] - pres
        rx = diff_axis(sxx, 0) + diff_axis(tau[3], 1) + diff_axis(tau[4], 2)
        rz = diff_axis(tau[3], 0) + diff_axis(szz, 1) + diff_axis(tau[5], 2)
        ry = diff_axis(tau[4], 0) + diff_axis(tau[5], 1) + diff_axis(syy, 2)
        velocity = velocity + step * jnp.stack([rx, rz, ry])
    return (velocity, pres, tau, plastic_sum, jnp.stack(peaks))
```

```python
import functools
import math

import jax
import jax.numpy as jnp
from jax import lax
from jax.experimental import pallas as pl
from jax.experimental.pallas import tpu as pltpu
from jax.sharding import PartitionSpec as P

ITERS = 2
REACH = 6
MESH = pl.DeviceIdType.MESH

unnormalized_weights = [math.exp(-(k * k) / 18.0) for k in range(-REACH, REACH + 1)]
weight_total = sum(unnormalized_weights)
gauss_weights = [value / weight_total for value in unnormalized_weights]
shear_time_increment = 20.0


def kernel(
    gx_count,
    gz_count,
    vel_in,
    pres_in,
    old_in,
    plas_in,
    visc_in,
    weak_in,
    vel_out,
    pres_out,
    stress_out,
    plas_out,
    peak_out,
    V,
    PR,
    OLD,
    PLX,
    VI,
    WK,
    ETA,
    COH,
    PL,
    YM,
    GX,
    GZH,
    SM,
    VZE,
    VZH,
    SX,
    TZ,
    SZE,
    SZH,
    RP,
    RH,
    R,
    RZE,
    RZH,
    TAU,
    PK,
    in_sem,
    out_sem,
    send_sem,
    recv_sem,
    pk_send,
    pk_recv,
):
    rows, nz, ny = PR.shape
    gx = lax.axis_index("gx")
    gz = lax.axis_index("gz")
    me = gx * gz_count + gz
    total = gx_count * gz_count
    has = {
        "xl": gx > 0,
        "xh": gx < gx_count - 1,
        "zl": gz > 0,
        "zh": gz < gz_count - 1,
    }
    target = {
        "xl": (gx - 1, gz),
        "xh": (gx + 1, gz),
        "zl": (gx, gz - 1),
        "zh": (gx, gz + 1),
    }
    opposite = {"xl": "xh", "xh": "xl", "zl": "zh", "zh": "zl"}

    barrier = pltpu.get_barrier_semaphore()

    def greet(step, carry):
        other = lax.rem(me + step, total)
        pl.semaphore_signal(
            barrier,
            inc=1,
            device_id=(other // gz_count, lax.rem(other, gz_count)),
            device_id_type=MESH,
        )
        return carry

    lax.fori_loop(1, total, greet, 0)

    loads = [
        pltpu.make_async_copy(plas_in, PLX.at[pl.ds(REACH, rows)], in_sem.at[0]),
        pltpu.make_async_copy(vel_in, V.at[:, pl.ds(1, rows)], in_sem.at[1]),
        pltpu.make_async_copy(visc_in, VI, in_sem.at[2]),
        pltpu.make_async_copy(weak_in, WK, in_sem.at[3]),
        pltpu.make_async_copy(old_in, OLD, in_sem.at[4]),
        pltpu.make_async_copy(pres_in, PR, in_sem.at[5]),
    ]
    for copy in loads:
        copy.start()

    count = [0]

    def exchange(side, source, landing):
        slot = count[0]
        count[0] += 1
        copy = pltpu.make_async_remote_copy(
            src_ref=source,
            dst_ref=landing,
            send_sem=send_sem.at[slot],
            recv_sem=recv_sem.at[slot],
            device_id=target[side],
            device_id_type=MESH,
        )

        @pl.when(has[side])
        def _():
            copy.start()

        return side, copy

    def wait_sent(pair):
        side, copy = pair

        @pl.when(has[side])
        def _():
            copy.wait_send()

    def wait_got(pair):
        side, copy = pair

        @pl.when(has[opposite[side]])
        def _():
            copy.wait_recv()

    def zero_unless(side, ref):
        @pl.when(jnp.logical_not(has[side]))
        def _():
            ref[...] = jnp.zeros(ref.shape, ref.dtype)

    zero_unless("xl", PLX.at[pl.ds(0, REACH)])
    zero_unless("xh", PLX.at[pl.ds(rows + REACH, REACH)])
    zero_unless("xl", V.at[:, pl.ds(0, 1)])
    zero_unless("xh", V.at[:, pl.ds(rows + 1, 1)])
    zero_unless("zl", GZH.at[0])
    zero_unless("zh", GZH.at[1])
    for buf in (VZH.at[0], RZH.at[0], SZH.at[0, 0], SZH.at[1, 0]):
        zero_unless("zl", buf)
    for buf in (VZH.at[1], RZH.at[1], SZH.at[0, 1], SZH.at[1, 1]):
        zero_unless("zh", buf)
    for it in range(ITERS):
        zero_unless("xl", SX.at[it, :, pl.ds(0, 1)])
        zero_unless("xh", SX.at[it, :, pl.ds(rows + 1, 1)])

    loads[0].wait()
    pl.semaphore_wait(barrier, total - 1)
    plas_copies = [
        exchange("xh", PLX.at[pl.ds(rows, REACH)], PLX.at[pl.ds(0, REACH)]),
        exchange("xl", PLX.at[pl.ds(REACH, REACH)], PLX.at[pl.ds(rows + REACH, REACH)]),
    ]
    loads[1].wait()
    vel_copies = [
        exchange("xh", V.at[:, pl.ds(rows, 1)], V.at[:, pl.ds(0, 1)]),
        exchange("xl", V.at[:, pl.ds(1, 1)], V.at[:, pl.ds(rows + 1, 1)]),
    ]

    def vel_edges(x, carry):
        for c in range(3):
            row = V[c, x + 1]
            VZE[0, c, x] = row[0:1]
            VZE[1, c, x] = row[nz - 1 : nz]
        return carry

    lax.fori_loop(0, rows, vel_edges, 0)
    vz_copies = [
        exchange("zh", VZE.at[1], VZH.at[0]),
        exchange("zl", VZE.at[0], VZH.at[1]),
    ]

    places_a = lax.broadcasted_iota(jnp.int32, (ny, ny), 0)
    places_b = lax.broadcasted_iota(jnp.int32, (ny, ny), 1)
    gap = (places_a - places_b).astype(jnp.float32)
    YM[...] = jnp.where(
        jnp.abs(gap) <= float(REACH), jnp.exp(-gap * gap / 18.0) / weight_total, 0.0
    )
    for copy in loads[2:]:
        copy.wait()

    def prepare(x, carry):
        eta = VI[x]
        ETA[x] = shear_time_increment * eta / (eta + shear_time_increment)
        return carry

    lax.fori_loop(0, rows, prepare, 0)

    sub = lax.broadcasted_iota(jnp.int32, (nz, ny), 0)
    lane = lax.broadcasted_iota(jnp.int32, (nz, ny), 1)

    for pair in plas_copies:
        wait_got(pair)

    def smooth_x(x, carry):
        total_ = gauss_weights[REACH] * PLX[x + REACH]
        for k in range(1, REACH + 1):
            total_ = total_ + gauss_weights[REACH + k] * (PLX[x + REACH - k] + PLX[x + REACH + k])
        GX[x] = total_
        PL[x] = PLX[x + REACH]
        return carry

    lax.fori_loop(0, rows, smooth_x, 0)
    gz_copies = [
        exchange("zh", GX, GZH.at[0]),
        exchange("zl", GX, GZH.at[1]),
    ]
    for pair in gz_copies:
        wait_got(pair)

    def smooth_z(x, carry):
        own, low, high = GX[x], GZH[0, x], GZH[1, x]
        total_ = gauss_weights[REACH] * own
        for k in range(1, REACH + 1):
            above = pltpu.roll(jnp.where(sub >= k, own, high), nz - k, 0)
            below = pltpu.roll(jnp.where(sub < nz - k, own, low), k, 0)
            total_ = total_ + gauss_weights[REACH + k] * (above + below)
        SM[pl.ds(pl.multiple_of(x * nz, nz), nz)] = total_
        return carry

    lax.fori_loop(0, rows, smooth_z, 0)
    smoothed = jnp.dot(SM[...], YM[...], precision=lax.Precision.HIGHEST, preferred_element_type=jnp.float32)
    SM[...] = smoothed

    def cohesion(x, carry):
        seeded = WK[x].astype(jnp.float32)
        value = SM[pl.ds(pl.multiple_of(x * nz, nz), nz)]
        COH[x] = 0.8660254 * ((1.0 - 0.6 * seeded) / (1.0 + 2.0 * value))
        return carry

    lax.fori_loop(0, rows, cohesion, 0)

    for pair in vel_copies + vz_copies:
        wait_got(pair)

    def dy(f):
        up = jnp.where(lane < ny - 1, pltpu.roll(f, ny - 1, 1), 0.0)
        down = jnp.where(lane > 0, pltpu.roll(f, 1, 1), 0.0)
        return (up - down) * 0.5

    def dz(f, low, high):
        up = pltpu.roll(jnp.where(sub >= 1, f, jnp.broadcast_to(high, f.shape)), nz - 1, 0)
        down = pltpu.roll(jnp.where(sub < nz - 1, f, jnp.broadcast_to(low, f.shape)), 1, 0)
        return (up - down) * 0.5

    stores = []
    for it in range(ITERS):
        last = it == ITERS - 1

        def stress_row(x, carry, it=it, last=last):
            most_f, most_eta = carry
            vx, vz, vy = V[0, x + 1], V[1, x + 1], V[2, x + 1]
            dx_v = [(V[c, x + 2] - V[c, x]) * 0.5 for c in range(3)]
            dz_v = [
                dz(f, VZH[0, c, x], VZH[1, c, x]) for c, f in enumerate((vx, vz, vy))
            ]
            dy_v = [dy(f) for f in (vx, vz, vy)]
            div = dx_v[0] + dz_v[1] + dy_v[2]
            third = div * (1.0 / 3.0)
            pres = PR[x] - 0.25 * div
            PR[x] = pres
            strain = (
                dx_v[0] - third,
                dz_v[1] - third,
                dy_v[2] - third,
                0.5 * (dx_v[1] + dz_v[0]),
                0.5 * (dx_v[2] + dy_v[0]),
                0.5 * (dz_v[2] + dy_v[1]),
            )
            eta = ETA[x]
            twice = 2.0 * eta
            trial = [
                twice * (strain[c] + OLD[c, x] * (0.5 / shear_time_increment)) for c in range(6)
            ]
            tau_ii = jnp.sqrt(
                0.5 * (trial[0] * trial[0] + trial[1] * trial[1] + trial[2] * trial[2])
                + trial[3] * trial[3]
                + trial[4] * trial[4]
                + trial[5] * trial[5]
            )
            yield_f = tau_ii - 0.5 * jnp.maximum(pres, 0.0) - COH[x]
            dlam = jnp.maximum(yield_f, 0.0) / (eta + 0.5)
            shrink = 1.0 - eta * dlam / jnp.maximum(tau_ii, 0.5)
            tau = [shrink * value for value in trial]
            PL[x] = PL[x] + dlam
            if last:
                for c in range(6):
                    TAU[c, x] = tau[c]
            SX[it, 0, x + 1] = tau[0] - pres
            SX[it, 1, x + 1] = tau[3]
            SX[it, 2, x + 1] = tau[4]
            szz = tau[1] - pres
            TZ[0, x] = szz
            TZ[1, x] = tau[5]
            TZ[2, x] = tau[2] - pres
            for c, f in enumerate((tau[3], szz, tau[5])):
                SZE[it, 0, c, x] = f[0:1]
                SZE[it, 1, c, x] = f[nz - 1 : nz]
            return jnp.maximum(most_f, yield_f), jnp.maximum(most_eta, eta * shrink)

        start = jnp.full((nz, ny), -jnp.inf, jnp.float32)
        most_f, most_eta = lax.fori_loop(0, rows, stress_row, (start, start))
        PK[it, me] = jnp.concatenate(
            [jnp.max(most_f, axis=0, keepdims=True), jnp.max(most_eta, axis=0, keepdims=True)],
            axis=0,
        )

        def tell(step, carry, it=it):
            other = lax.rem(me + step, total)
            pltpu.make_async_remote_copy(
                src_ref=PK.at[it, me],
                dst_ref=PK.at[it, me],
                send_sem=pk_send.at[it],
                recv_sem=pk_recv.at[it],
                device_id=(other // gz_count, lax.rem(other, gz_count)),
                device_id_type=MESH,
            ).start()
            return carry

        lax.fori_loop(1, total, tell, 0)
        sx_copies = [
            exchange("xh", SX.at[it, :, pl.ds(rows, 1)], SX.at[it, :, pl.ds(0, 1)]),
            exchange("xl", SX.at[it, :, pl.ds(1, 1)], SX.at[it, :, pl.ds(rows + 1, 1)]),
        ]
        sz_copies = [
            exchange("zh", SZE.at[it, 1], SZH.at[it, 0]),
            exchange("zl", SZE.at[it, 0], SZH.at[it, 1]),
        ]
        if last:
            stores += [
                pltpu.make_async_copy(TAU, stress_out, out_sem.at[0]),
                pltpu.make_async_copy(PR, pres_out, out_sem.at[1]),
                pltpu.make_async_copy(PL, plas_out, out_sem.at[2]),
            ]
            for copy in stores:
                copy.start()

        for pair in sz_copies:
            wait_got(pair)

        def in_row(x, it=it):
            txz, txy = SX[it, 1, x + 1], SX[it, 2, x + 1]
            szz, tzy, syy = TZ[0, x], TZ[1, x], TZ[2, x]
            z_terms = [
                dz(f, SZH[it, 0, c, x], SZH[it, 1, c, x]) for c, f in enumerate((txz, szz, tzy))
            ]
            y_terms = [dy(f) for f in (txy, tzy, syy)]
            return [a + b for a, b in zip(z_terms, y_terms)]

        r_copies = []
        if not last:
            low_row, high_row = in_row(0), in_row(rows - 1)
            for c in range(3):
                RP[0, c] = low_row[c] + 0.5 * SX[it, c, 2]
                RP[1, c] = high_row[c] - 0.5 * SX[it, c, rows - 1]
            r_copies += [
                exchange("xh", RP.at[1], RH.at[0]),
                exchange("xl", RP.at[0], RH.at[1]),
            ]
        for pair in sx_copies:
            wait_got(pair)

        def residual_row(x, carry, it=it, last=last):
            terms = in_row(x)
            for c in range(3):
                value = terms[c] + (SX[it, c, x + 2] - SX[it, c, x]) * 0.5
                R[c, x] = value
                if not last:
                    RZE[0, c, x] = value[0:1]
                    RZE[1, c, x] = value[nz - 1 : nz]
            return carry

        lax.fori_loop(0, rows, residual_row, 0)
        if not last:
            r_copies += [
                exchange("zh", RZE.at[1], RZH.at[0]),
                exchange("zl", RZE.at[0], RZH.at[1]),
            ]
            for pair in vel_copies:
                wait_sent(pair)
            for pair in r_copies:
                wait_got(pair)

        others = PK.at[it, pl.ds(0, total - 1)]
        arrived = pltpu.make_async_copy(others, others, pk_recv.at[it])
        arrived.wait()
        peaks = jnp.max(PK[it], axis=0)
        step = 0.125 / jnp.max(peaks[1:2], axis=1, keepdims=True)

        def velocity_row(x, carry):
            for c in range(3):
                V[c, x + 1] = V[c, x + 1] + step * R[c, x]
            return carry

        lax.fori_loop(0, rows, velocity_row, 0)
        if last:
            copy = pltpu.make_async_copy(V.at[:, pl.ds(1, rows)], vel_out, out_sem.at[3])
            copy.start()
            stores.append(copy)
        else:

            @pl.when(has["xl"])
            def _(it=it, step=step):
                for c in range(3):
                    V[c, 0] = V[c, 0] + step * (RH[0, c] + 0.5 * SX[it, c, 1])

            @pl.when(has["xh"])
            def _(it=it, step=step):
                for c in range(3):
                    V[c, rows + 1] = V[c, rows + 1] + step * (RH[1, c] - 0.5 * SX[it, c, rows])

            def edge_row(x, carry):
                for c in range(3):
                    for side in range(2):
                        VZH[side, c, x] = VZH[side, c, x] + step * RZH[side, c, x]
                return carry

            lax.fori_loop(0, rows, edge_row, 0)
        peak_out[it] = jnp.max(peaks[0:1])
        for pair in sx_copies + sz_copies + r_copies:
            wait_sent(pair)
        pltpu.make_async_copy(others, others, pk_send.at[it]).wait()

    for pair in plas_copies + vz_copies + gz_copies:
        wait_sent(pair)
    for copy in stores:
        copy.wait()


def solution(mesh):
    gx_count, gz_count = mesh.shape["gx"], mesh.shape["gz"]
    total = gx_count * gz_count

    def per_device(velocity, pressure, stress_old, plastic, viscosity, weak_seed):
        rows, nz, ny = pressure.shape
        cells = (rows, nz, ny)
        f32 = jnp.float32
        vm = lambda *shape: pltpu.VMEM(shape, f32)
        copies = 6 + 2 + 4 * ITERS + 4 * (ITERS - 1)
        anywhere = pl.BlockSpec(memory_space=pl.ANY)
        return pl.pallas_call(
            functools.partial(kernel, gx_count, gz_count),
            out_shape=(
                jax.ShapeDtypeStruct(velocity.shape, f32),
                jax.ShapeDtypeStruct(pressure.shape, f32),
                jax.ShapeDtypeStruct(stress_old.shape, f32),
                jax.ShapeDtypeStruct(plastic.shape, f32),
                jax.ShapeDtypeStruct((ITERS,), f32),
            ),
            in_specs=[anywhere] * 6,
            out_specs=(anywhere,) * 4 + (pl.BlockSpec(memory_space=pltpu.SMEM),),
            scratch_shapes=[
                vm(3, rows + 2, nz, ny),
                vm(*cells),
                vm(6, *cells),
                vm(rows + 2 * REACH, nz, ny),
                vm(*cells),
                pltpu.VMEM(cells, jnp.int32),
                vm(*cells),
                vm(*cells),
                vm(*cells),
                vm(ny, ny),
                vm(*cells),
                vm(2, *cells),
                vm(rows * nz, ny),
                vm(2, 3, rows, 1, ny),
                vm(2, 3, rows, 1, ny),
                vm(ITERS, 3, rows + 2, nz, ny),
                vm(3, *cells),
                vm(ITERS, 2, 3, rows, 1, ny),
                vm(ITERS, 2, 3, rows, 1, ny),
                vm(2, 3, nz, ny),
                vm(2, 3, nz, ny),
                vm(3, *cells),
                vm(2, 3, rows, 1, ny),
                vm(2, 3, rows, 1, ny),
                vm(6, *cells),
                vm(ITERS, total, 2, ny),
                pltpu.SemaphoreType.DMA((6,)),
                pltpu.SemaphoreType.DMA((4,)),
                pltpu.SemaphoreType.DMA((copies,)),
                pltpu.SemaphoreType.DMA((copies,)),
                pltpu.SemaphoreType.DMA((ITERS,)),
                pltpu.SemaphoreType.DMA((ITERS,)),
            ],
            compiler_params=pltpu.CompilerParams(collective_id=0, has_side_effects=True),
        )(velocity, pressure, stress_old, plastic, viscosity, weak_seed)

    in_specs = (
        P(None, "gx", "gz", None),
        P("gx", "gz", None),
        P(None, "gx", "gz", None),
        P("gx", "gz", None),
        P("gx", "gz", None),
        P("gx", "gz", None),
    )
    out_specs = (
        P(None, "gx", "gz", None),
        P("gx", "gz", None),
        P(None, "gx", "gz", None),
        P("gx", "gz", None),
        P(),
    )
    return jax.shard_map(
        per_device, mesh=mesh, in_specs=in_specs, out_specs=out_specs, check_vma=False
    )
```

```python
import functools
import math

import jax
import jax.numpy as jnp
from jax import lax
from jax.experimental import pallas as pl
from jax.experimental.pallas import tpu as pltpu
from jax.sharding import PartitionSpec as P

ITERS = 2
REACH = 6
BLOCK = 2
MESH = pl.DeviceIdType.MESH

unnormalized_weights = [math.exp(-(k * k) / 18.0) for k in range(-REACH, REACH + 1)]
weight_total = sum(unnormalized_weights)
gauss_weights = [value / weight_total for value in unnormalized_weights]
shear_time_increment = 20.0


def kernel(
    gx_count,
    gz_count,
    vel_in,
    pres_in,
    old_in,
    plas_in,
    visc_in,
    weak_in,
    VOUT,
    PR,
    TAU,
    PL,
    peak_out,
    V,
    PIN,
    OLD,
    PLX,
    VI,
    WK,
    ETA,
    COH,
    YM,
    GX,
    GZH,
    SM,
    VZE,
    VZH,
    SX,
    TZ,
    SZE,
    SZH,
    RP,
    RH,
    R,
    RZE,
    RZH,
    TB,
    PK,
    in_sem,
    send_sem,
    recv_sem,
    pk_send,
    pk_recv,
):
    rows, nz, ny = PR.shape
    gx = lax.axis_index("gx")
    gz = lax.axis_index("gz")
    me = gx * gz_count + gz
    total = gx_count * gz_count
    has = {
        "xl": gx > 0,
        "xh": gx < gx_count - 1,
        "zl": gz > 0,
        "zh": gz < gz_count - 1,
    }
    target = {
        "xl": (gx - 1, gz),
        "xh": (gx + 1, gz),
        "zl": (gx, gz - 1),
        "zh": (gx, gz + 1),
    }
    opposite = {"xl": "xh", "xh": "xl", "zl": "zh", "zh": "zl"}

    barrier = pltpu.get_barrier_semaphore()

    def greet(step, carry):
        other = lax.rem(me + step, total)
        pl.semaphore_signal(
            barrier,
            inc=1,
            device_id=(other // gz_count, lax.rem(other, gz_count)),
            device_id_type=MESH,
        )
        return carry

    lax.fori_loop(1, total, greet, 0)

    loads = [
        pltpu.make_async_copy(plas_in, PLX.at[pl.ds(REACH, rows)], in_sem.at[0]),
        pltpu.make_async_copy(vel_in, V.at[:, pl.ds(1, rows)], in_sem.at[1]),
        pltpu.make_async_copy(visc_in, VI, in_sem.at[2]),
        pltpu.make_async_copy(weak_in, WK, in_sem.at[3]),
        pltpu.make_async_copy(old_in, OLD, in_sem.at[4]),
        pltpu.make_async_copy(pres_in, PIN, in_sem.at[5]),
    ]
    for copy in loads:
        copy.start()

    count = [0]

    def exchange(side, source, landing):
        slot = count[0]
        count[0] += 1
        copy = pltpu.make_async_remote_copy(
            src_ref=source,
            dst_ref=landing,
            send_sem=send_sem.at[slot],
            recv_sem=recv_sem.at[slot],
            device_id=target[side],
            device_id_type=MESH,
        )

        @pl.when(has[side])
        def _():
            copy.start()

        return side, copy

    def wait_sent(pair):
        side, copy = pair

        @pl.when(has[side])
        def _():
            copy.wait_send()

    def wait_got(pair):
        side, copy = pair

        @pl.when(has[opposite[side]])
        def _():
            copy.wait_recv()

    def zero_unless(side, ref):
        @pl.when(jnp.logical_not(has[side]))
        def _():
            ref[...] = jnp.zeros(ref.shape, ref.dtype)

    zero_unless("xl", PLX.at[pl.ds(0, REACH)])
    zero_unless("xh", PLX.at[pl.ds(rows + REACH, REACH)])
    zero_unless("xl", V.at[:, pl.ds(0, 1)])
    zero_unless("xh", V.at[:, pl.ds(rows + 1, 1)])
    zero_unless("zl", GZH.at[0])
    zero_unless("zh", GZH.at[1])
    for buf in (VZH.at[0], RZH.at[0], SZH.at[0, 0], SZH.at[1, 0]):
        zero_unless("zl", buf)
    for buf in (VZH.at[1], RZH.at[1], SZH.at[0, 1], SZH.at[1, 1]):
        zero_unless("zh", buf)
    for it in range(ITERS):
        zero_unless("xl", SX.at[it, :, pl.ds(0, 1)])
        zero_unless("xh", SX.at[it, :, pl.ds(rows + 1, 1)])

    loads[0].wait()
    pl.semaphore_wait(barrier, total - 1)
    plas_copies = [
        exchange("xh", PLX.at[pl.ds(rows, REACH)], PLX.at[pl.ds(0, REACH)]),
        exchange("xl", PLX.at[pl.ds(REACH, REACH)], PLX.at[pl.ds(rows + REACH, REACH)]),
    ]
    loads[1].wait()
    vel_copies = [
        exchange("xh", V.at[:, pl.ds(rows, 1)], V.at[:, pl.ds(0, 1)]),
        exchange("xl", V.at[:, pl.ds(1, 1)], V.at[:, pl.ds(rows + 1, 1)]),
    ]

    def vel_edges(x, carry):
        for c in range(3):
            row = V[c, x + 1]
            VZE[0, c, x] = row[0:1]
            VZE[1, c, x] = row[nz - 1 : nz]
        return carry

    lax.fori_loop(0, rows, vel_edges, 0)
    vz_copies = [
        exchange("zh", VZE.at[1], VZH.at[0]),
        exchange("zl", VZE.at[0], VZH.at[1]),
    ]

    places_a = lax.broadcasted_iota(jnp.int32, (ny, ny), 0)
    places_b = lax.broadcasted_iota(jnp.int32, (ny, ny), 1)
    gap = (places_a - places_b).astype(jnp.float32)
    YM[...] = jnp.where(
        jnp.abs(gap) <= float(REACH), jnp.exp(-gap * gap / 18.0) / weight_total, 0.0
    )
    for copy in loads[2:]:
        copy.wait()

    def prepare(x, carry):
        eta = VI[x]
        ETA[x] = shear_time_increment * eta / (eta + shear_time_increment)
        return carry

    lax.fori_loop(0, rows, prepare, 0)

    block = next(size for size in (BLOCK, 2, 1) if rows % size == 0)
    many = (block, nz, ny)
    sub = lax.broadcasted_iota(jnp.int32, many, 1)
    lane = lax.broadcasted_iota(jnp.int32, many, 2)

    def over_rows(body, carry=0):
        return lax.fori_loop(0, rows // block, lambda i, state: body(i * block, state), carry)

    def at(x):
        return pl.ds(x, block)

    for pair in plas_copies:
        wait_got(pair)

    def smooth_x(x, carry):
        sum_ = gauss_weights[REACH] * PLX[at(x + REACH)]
        for k in range(1, REACH + 1):
            sum_ = sum_ + gauss_weights[REACH + k] * (PLX[at(x + REACH - k)] + PLX[at(x + REACH + k)])
        GX[at(x)] = sum_
        return carry

    over_rows(smooth_x)
    gz_copies = [
        exchange("zh", GX, GZH.at[0]),
        exchange("zl", GX, GZH.at[1]),
    ]
    for pair in vel_copies + vz_copies:
        wait_got(pair)

    def dy(f):
        up = jnp.where(lane < ny - 1, pltpu.roll(f, ny - 1, 2), 0.0)
        down = jnp.where(lane > 0, pltpu.roll(f, 1, 2), 0.0)
        return (up - down) * 0.5

    def dz(f, low, high):
        up = pltpu.roll(jnp.where(sub >= 1, f, jnp.broadcast_to(high, f.shape)), nz - 1, 1)
        down = pltpu.roll(jnp.where(sub < nz - 1, f, jnp.broadcast_to(low, f.shape)), 1, 1)
        return (up - down) * 0.5

    def trial_stress(x, pres):
        v = [V[c, at(x + 1)] for c in range(3)]
        dx_v = [(V[c, at(x + 2)] - V[c, at(x)]) * 0.5 for c in range(3)]
        dz_v = [dz(f, VZH[0, c, at(x)], VZH[1, c, at(x)]) for c, f in enumerate(v)]
        dy_v = [dy(f) for f in v]
        div = dx_v[0] + dz_v[1] + dy_v[2]
        third = div * (1.0 / 3.0)
        pres = pres - 0.25 * div
        PR[at(x)] = pres
        strain = (
            dx_v[0] - third,
            dz_v[1] - third,
            dy_v[2] - third,
            0.5 * (dx_v[1] + dz_v[0]),
            0.5 * (dx_v[2] + dy_v[0]),
            0.5 * (dz_v[2] + dy_v[1]),
        )
        twice = 2.0 * ETA[at(x)]
        trial = [
            twice * (strain[c] + OLD[c, at(x)] * (0.5 / shear_time_increment)) for c in range(6)
        ]
        tau_ii = jnp.sqrt(
            0.5 * (trial[0] * trial[0] + trial[1] * trial[1] + trial[2] * trial[2])
            + trial[3] * trial[3]
            + trial[4] * trial[4]
            + trial[5] * trial[5]
        )
        return pres, trial, tau_ii

    def first_trial(x, carry):
        _, trial, tau_ii = trial_stress(x, PIN[at(x)])
        for c in range(6):
            TAU[c, at(x)] = trial[c]
        TB[at(x)] = tau_ii
        return carry

    over_rows(first_trial)

    for pair in gz_copies:
        wait_got(pair)

    def smooth_z(x, carry):
        own, low, high = GX[at(x)], GZH[0, at(x)], GZH[1, at(x)]
        sum_ = gauss_weights[REACH] * own
        for k in range(1, REACH + 1):
            above = pltpu.roll(jnp.where(sub >= k, own, high), nz - k, 1)
            below = pltpu.roll(jnp.where(sub < nz - k, own, low), k, 1)
            sum_ = sum_ + gauss_weights[REACH + k] * (above + below)
        SM[at(x)] = sum_
        return carry

    over_rows(smooth_z)
    SM[...] = jnp.dot(
        SM[...].reshape(rows * nz, ny),
        YM[...],
        precision=lax.Precision.HIGHEST,
        preferred_element_type=jnp.float32,
    ).reshape(rows, nz, ny)

    half = ny // 2 if ny % 256 == 0 else ny
    for it in range(ITERS):
        last = it == ITERS - 1

        def stress_row(x, carry, it=it, last=last):
            most_f, most_eta = carry
            if it == 0:
                pres, trial, tau_ii = PR[at(x)], [TAU[c, at(x)] for c in range(6)], TB[at(x)]
                seeded = WK[at(x)].astype(jnp.float32)
                strength = 0.8660254 * ((1.0 - 0.6 * seeded) / (1.0 + 2.0 * SM[at(x)]))
                COH[at(x)] = strength
                plas = PLX[at(x + REACH)]
            else:
                pres, trial, tau_ii = trial_stress(x, PR[at(x)])
                strength = COH[at(x)]
                plas = PL[at(x)]
            eta = ETA[at(x)]
            yield_f = tau_ii - 0.5 * jnp.maximum(pres, 0.0) - strength
            dlam = jnp.maximum(yield_f, 0.0) / (eta + 0.5)
            shrink = 1.0 - eta * dlam / jnp.maximum(tau_ii, 0.5)
            tau = [shrink * value for value in trial]
            PL[at(x)] = plas + dlam
            if last:
                for c in range(6):
                    TAU[c, at(x)] = tau[c]
            SX[it, 0, at(x + 1)] = tau[0] - pres
            SX[it, 1, at(x + 1)] = tau[3]
            SX[it, 2, at(x + 1)] = tau[4]
            szz = tau[1] - pres
            TZ[0, at(x)] = szz
            TZ[1, at(x)] = tau[5]
            TZ[2, at(x)] = tau[2] - pres
            for c, f in enumerate((tau[3], szz, tau[5])):
                SZE[it, 0, c, at(x)] = f[:, 0:1]
                SZE[it, 1, c, at(x)] = f[:, nz - 1 : nz]
            return jnp.maximum(most_f, yield_f), jnp.maximum(most_eta, eta * shrink)

        start = jnp.full(many, -jnp.inf, jnp.float32)
        most_f, most_eta = over_rows(stress_row, (start, start))
        sx_copies = [
            exchange("xh", SX.at[it, :, pl.ds(rows, 1)], SX.at[it, :, pl.ds(0, 1)]),
            exchange("xl", SX.at[it, :, pl.ds(1, 1)], SX.at[it, :, pl.ds(rows + 1, 1)]),
        ]
        sz_copies = [
            exchange("zh", SZE.at[it, 1], SZH.at[it, 0]),
            exchange("zl", SZE.at[it, 0], SZH.at[it, 1]),
        ]

        def folded(most):
            most = jnp.max(jnp.max(most, axis=0), axis=0, keepdims=True)
            return jnp.maximum(most[:, :half], most[:, ny - half :])

        PK[it, me] = jnp.concatenate([folded(most_f), folded(most_eta)], axis=0)

        def tell(step, carry, it=it):
            other = lax.rem(me + step, total)
            pltpu.make_async_remote_copy(
                src_ref=PK.at[it, me],
                dst_ref=PK.at[it, me],
                send_sem=pk_send.at[it],
                recv_sem=pk_recv.at[it],
                device_id=(other // gz_count, lax.rem(other, gz_count)),
                device_id_type=MESH,
            ).start()
            return carry

        lax.fori_loop(1, total, tell, 0)
        for pair in sz_copies:
            wait_got(pair)

        def inner_row(x, carry, it=it):
            txz, txy = SX[it, 1, at(x + 1)], SX[it, 2, at(x + 1)]
            szz, tzy, syy = TZ[0, at(x)], TZ[1, at(x)], TZ[2, at(x)]
            z_terms = [
                dz(f, SZH[it, 0, c, at(x)], SZH[it, 1, c, at(x)])
                for c, f in enumerate((txz, szz, tzy))
            ]
            y_terms = [dy(f) for f in (txy, tzy, syy)]
            for c in range(3):
                R[c, at(x)] = z_terms[c] + y_terms[c]
            return carry

        def add_x(low, high, it=it):
            for c in range(3):
                R[c, low:high] = R[c, low:high] + 0.5 * (
                    SX[it, c, low + 2 : high + 2] - SX[it, c, low:high]
                )

        r_copies = []
        if not last:
            inner_row(0, 0)
            inner_row(rows - block, 0)
            for c in range(3):
                RP[0, c] = R[c, 0] + 0.5 * SX[it, c, 2]
                RP[1, c] = R[c, rows - 1] - 0.5 * SX[it, c, rows - 1]
            r_copies += [
                exchange("xh", RP.at[1], RH.at[0]),
                exchange("xl", RP.at[0], RH.at[1]),
            ]
        over_rows(inner_row)
        add_x(1, rows - 1)
        for pair in sx_copies:
            wait_got(pair)
        add_x(0, 1)
        add_x(rows - 1, rows)
        if not last:

            def edges(x, carry):
                for c in range(3):
                    value = R[c, at(x)]
                    RZE[0, c, at(x)] = value[:, 0:1]
                    RZE[1, c, at(x)] = value[:, nz - 1 : nz]
                return carry

            over_rows(edges)
            r_copies += [
                exchange("zh", RZE.at[1], RZH.at[0]),
                exchange("zl", RZE.at[0], RZH.at[1]),
            ]
            for pair in vel_copies:
                wait_sent(pair)
            for pair in r_copies:
                wait_got(pair)

        others = PK.at[it, pl.ds(0, total - 1)]
        arrived = pltpu.make_async_copy(others, others, pk_recv.at[it])
        arrived.wait()
        peaks = jnp.max(PK[it], axis=0)
        step = 0.125 / jnp.max(peaks[1:2], axis=1, keepdims=True)

        def velocity_row(x, carry):
            for c in range(3):
                value = V[c, at(x + 1)] + step * R[c, at(x)]
                if last:
                    VOUT[c, at(x)] = value
                else:
                    V[c, at(x + 1)] = value
            return carry

        over_rows(velocity_row)
        if not last:

            @pl.when(has["xl"])
            def _(it=it, step=step):
                for c in range(3):
                    V[c, 0] = V[c, 0] + step * (RH[0, c] + 0.5 * SX[it, c, 1])

            @pl.when(has["xh"])
            def _(it=it, step=step):
                for c in range(3):
                    V[c, rows + 1] = V[c, rows + 1] + step * (RH[1, c] - 0.5 * SX[it, c, rows])

            VZH[...] = VZH[...] + step * RZH[...]
        peak_out[it] = jnp.max(peaks[0:1])
        for pair in sx_copies + sz_copies + r_copies:
            wait_sent(pair)
        pltpu.make_async_copy(others, others, pk_send.at[it]).wait()

    for pair in plas_copies + vz_copies + gz_copies:
        wait_sent(pair)


def store_kernel(*refs):
    held, out, sem = refs[:5], refs[5:10], refs[10]
    copies = [pltpu.make_async_copy(a, b, sem.at[i]) for i, (a, b) in enumerate(zip(held, out))]
    for copy in copies:
        copy.start()
    for copy in copies:
        copy.wait()


def solution(mesh):
    gx_count, gz_count = mesh.shape["gx"], mesh.shape["gz"]
    total = gx_count * gz_count

    def per_device(velocity, pressure, stress_old, plastic, viscosity, weak_seed):
        rows, nz, ny = pressure.shape
        cells = (rows, nz, ny)
        f32 = jnp.float32
        vm = lambda *shape: pltpu.VMEM(shape, f32)
        copies = 6 + 2 + 4 * ITERS + 4 * (ITERS - 1)
        anywhere = pl.BlockSpec(memory_space=pl.ANY)
        shapes = (velocity.shape, pressure.shape, stress_old.shape, plastic.shape)
        *held, peaks = pl.pallas_call(
            functools.partial(kernel, gx_count, gz_count),
            out_shape=tuple(vm(*shape) for shape in shapes)
            + (jax.ShapeDtypeStruct((ITERS,), f32),),
            in_specs=[anywhere] * 6,
            out_specs=(pl.BlockSpec(memory_space=pltpu.VMEM),) * 4
            + (pl.BlockSpec(memory_space=pltpu.SMEM),),
            scratch_shapes=[
                vm(3, rows + 2, nz, ny),
                vm(*cells),
                vm(6, *cells),
                vm(rows + 2 * REACH, nz, ny),
                vm(*cells),
                pltpu.VMEM(cells, jnp.int32),
                vm(*cells),
                vm(*cells),
                vm(ny, ny),
                vm(*cells),
                vm(2, *cells),
                vm(*cells),
                vm(2, 3, rows, 1, ny),
                vm(2, 3, rows, 1, ny),
                vm(ITERS, 3, rows + 2, nz, ny),
                vm(3, *cells),
                vm(ITERS, 2, 3, rows, 1, ny),
                vm(ITERS, 2, 3, rows, 1, ny),
                vm(2, 3, nz, ny),
                vm(2, 3, nz, ny),
                vm(3, *cells),
                vm(2, 3, rows, 1, ny),
                vm(2, 3, rows, 1, ny),
                vm(*cells),
                vm(ITERS, total, 2, ny // 2 if ny % 256 == 0 else ny),
                pltpu.SemaphoreType.DMA((6,)),
                pltpu.SemaphoreType.DMA((copies,)),
                pltpu.SemaphoreType.DMA((copies,)),
                pltpu.SemaphoreType.DMA((ITERS,)),
                pltpu.SemaphoreType.DMA((ITERS,)),
            ],
            compiler_params=pltpu.CompilerParams(collective_id=0, has_side_effects=True),
        )(velocity, pressure, stress_old, plastic, viscosity, weak_seed)
        held = [pltpu.with_memory_space_constraint(array, pltpu.VMEM) for array in held]
        return pl.pallas_call(
            store_kernel,
            out_shape=tuple(jax.ShapeDtypeStruct(shape, f32) for shape in shapes)
            + (jax.ShapeDtypeStruct((ITERS,), f32),),
            in_specs=[anywhere] * 5,
            out_specs=(anywhere,) * 5,
            scratch_shapes=[pltpu.SemaphoreType.DMA((5,))],
        )(*held, peaks)

    in_specs = (
        P(None, "gx", "gz", None),
        P("gx", "gz", None),
        P(None, "gx", "gz", None),
        P("gx", "gz", None),
        P("gx", "gz", None),
        P("gx", "gz", None),
    )
    out_specs = (
        P(None, "gx", "gz", None),
        P("gx", "gz", None),
        P(None, "gx", "gz", None),
        P("gx", "gz", None),
        P(),
    )
    return jax.shard_map(
        per_device, mesh=mesh, in_specs=in_specs, out_specs=out_specs, check_vma=False
    )
```

```python
import functools
import math

import jax
import jax.numpy as jnp
from jax import lax
from jax.experimental import pallas as pl
from jax.experimental.pallas import tpu as pltpu
from jax.sharding import PartitionSpec as P

ITERS = 2
REACH = 6
BLOCK = 2
UNROLL = 1
MESH = pl.DeviceIdType.MESH

unnormalized_weights = [math.exp(-(k * k) / 18.0) for k in range(-REACH, REACH + 1)]
weight_total = sum(unnormalized_weights)
gauss_weights = [value / weight_total for value in unnormalized_weights]
shear_time_increment = 20.0


def kernel(
    gx_count,
    gz_count,
    vel_in,
    pres_in,
    old_in,
    plas_in,
    visc_in,
    weak_in,
    VOUT,
    PR,
    TAU,
    PL,
    peak_out,
    V,
    PIN,
    OLD,
    PLX,
    VI,
    WK,
    ETA,
    COH,
    YM,
    GX,
    GZH,
    SM,
    VZE,
    VZH,
    SX,
    TZ,
    SZE,
    SZH,
    RP,
    RH,
    R,
    RZE,
    RZH,
    TB,
    PK,
    in_sem,
    send_sem,
    recv_sem,
    pk_send,
    pk_recv,
):
    rows, nz, ny = PR.shape
    gx = lax.axis_index("gx")
    gz = lax.axis_index("gz")
    me = gx * gz_count + gz
    total = gx_count * gz_count
    has = {
        "xl": gx > 0,
        "xh": gx < gx_count - 1,
        "zl": gz > 0,
        "zh": gz < gz_count - 1,
    }
    target = {
        "xl": (gx - 1, gz),
        "xh": (gx + 1, gz),
        "zl": (gx, gz - 1),
        "zh": (gx, gz + 1),
    }
    opposite = {"xl": "xh", "xh": "xl", "zl": "zh", "zh": "zl"}

    barrier = pltpu.get_barrier_semaphore()

    def to_others(act):
        for dz_ in range(gz_count):
            other_z = gz + dz_
            other_z = jnp.where(other_z >= gz_count, other_z - gz_count, other_z)

            def body(dx_, carry):
                other_x = gx + dx_
                act((jnp.where(other_x >= gx_count, other_x - gx_count, other_x), other_z))
                return carry

            lax.fori_loop(0 if dz_ else 1, gx_count, body, 0, unroll=UNROLL)

    loads = [
        pltpu.make_async_copy(plas_in, PLX.at[pl.ds(REACH, rows)], in_sem.at[0]),
        pltpu.make_async_copy(vel_in, V.at[:, pl.ds(1, rows)], in_sem.at[1]),
        pltpu.make_async_copy(visc_in, VI, in_sem.at[2]),
        pltpu.make_async_copy(weak_in, WK, in_sem.at[3]),
        pltpu.make_async_copy(old_in, OLD, in_sem.at[4]),
        pltpu.make_async_copy(pres_in, PIN, in_sem.at[5]),
    ]
    for copy in loads[:2]:
        copy.start()
    to_others(
        lambda place: pl.semaphore_signal(
            barrier, inc=1, device_id=place, device_id_type=MESH
        )
    )
    for copy in loads[2:]:
        copy.start()

    count = [0]

    def exchange(side, source, landing):
        slot = count[0]
        count[0] += 1
        copy = pltpu.make_async_remote_copy(
            src_ref=source,
            dst_ref=landing,
            send_sem=send_sem.at[slot],
            recv_sem=recv_sem.at[slot],
            device_id=target[side],
            device_id_type=MESH,
        )

        @pl.when(has[side])
        def _():
            copy.start()

        return side, copy

    def wait_sent(pair):
        side, copy = pair

        @pl.when(has[side])
        def _():
            copy.wait_send()

    def wait_got(pair):
        side, copy = pair

        @pl.when(has[opposite[side]])
        def _():
            copy.wait_recv()

    def zero_unless(side, ref):
        @pl.when(jnp.logical_not(has[side]))
        def _():
            ref[...] = jnp.zeros(ref.shape, ref.dtype)

    zero_unless("xl", PLX.at[pl.ds(0, REACH)])
    zero_unless("xh", PLX.at[pl.ds(rows + REACH, REACH)])
    zero_unless("xl", V.at[:, pl.ds(0, 1)])
    zero_unless("xh", V.at[:, pl.ds(rows + 1, 1)])
    zero_unless("zl", GZH.at[0])
    zero_unless("zh", GZH.at[1])
    for buf in (VZH.at[0], RZH.at[0], SZH.at[0, 0], SZH.at[1, 0]):
        zero_unless("zl", buf)
    for buf in (VZH.at[1], RZH.at[1], SZH.at[0, 1], SZH.at[1, 1]):
        zero_unless("zh", buf)
    for it in range(ITERS):
        zero_unless("xl", SX.at[it, :, pl.ds(0, 1)])
        zero_unless("xh", SX.at[it, :, pl.ds(rows + 1, 1)])

    loads[0].wait()
    loads[1].wait()

    def vel_edges(x, carry):
        for c in range(3):
            row = V[c, x + 1]
            VZE[0, c, x] = row[0:1]
            VZE[1, c, x] = row[nz - 1 : nz]
        return carry

    lax.fori_loop(0, rows, vel_edges, 0)
    pl.semaphore_wait(barrier, total - 1)
    plas_copies = [
        exchange("xh", PLX.at[pl.ds(rows, REACH)], PLX.at[pl.ds(0, REACH)]),
        exchange("xl", PLX.at[pl.ds(REACH, REACH)], PLX.at[pl.ds(rows + REACH, REACH)]),
    ]
    vel_copies = [
        exchange("xh", V.at[:, pl.ds(rows, 1)], V.at[:, pl.ds(0, 1)]),
        exchange("xl", V.at[:, pl.ds(1, 1)], V.at[:, pl.ds(rows + 1, 1)]),
    ]

    vz_copies = [
        exchange("zh", VZE.at[1], VZH.at[0]),
        exchange("zl", VZE.at[0], VZH.at[1]),
    ]

    places_a = lax.broadcasted_iota(jnp.int32, (ny, ny), 0)
    places_b = lax.broadcasted_iota(jnp.int32, (ny, ny), 1)
    gap = (places_a - places_b).astype(jnp.float32)
    YM[...] = jnp.where(
        jnp.abs(gap) <= float(REACH), jnp.exp(-gap * gap / 18.0) / weight_total, 0.0
    )
    for copy in loads[2:]:
        copy.wait()

    def prepare(x, carry):
        eta = VI[x]
        ETA[x] = shear_time_increment * eta / (eta + shear_time_increment)
        return carry

    lax.fori_loop(0, rows, prepare, 0)

    block = next(size for size in (BLOCK, 2, 1) if rows % size == 0)
    many = (block, nz, ny)
    sub = lax.broadcasted_iota(jnp.int32, many, 1)
    lane = lax.broadcasted_iota(jnp.int32, many, 2)

    def over_rows(body, carry=0):
        return lax.fori_loop(0, rows // block, lambda i, state: body(i * block, state), carry)

    def at(x):
        return pl.ds(x, block)

    for pair in plas_copies:
        wait_got(pair)

    def smooth_x(x, carry):
        sum_ = gauss_weights[REACH] * PLX[at(x + REACH)]
        for k in range(1, REACH + 1):
            sum_ = sum_ + gauss_weights[REACH + k] * (PLX[at(x + REACH - k)] + PLX[at(x + REACH + k)])
        GX[at(x)] = sum_
        return carry

    over_rows(smooth_x)
    gz_copies = [
        exchange("zh", GX, GZH.at[0]),
        exchange("zl", GX, GZH.at[1]),
    ]
    for pair in vel_copies + vz_copies:
        wait_got(pair)

    def dy(f):
        up = jnp.where(lane < ny - 1, pltpu.roll(f, ny - 1, 2), 0.0)
        down = jnp.where(lane > 0, pltpu.roll(f, 1, 2), 0.0)
        return (up - down) * 0.5

    def dz(f, low, high):
        up = pltpu.roll(jnp.where(sub >= 1, f, jnp.broadcast_to(high, f.shape)), nz - 1, 1)
        down = pltpu.roll(jnp.where(sub < nz - 1, f, jnp.broadcast_to(low, f.shape)), 1, 1)
        return (up - down) * 0.5

    def trial_stress(x, pres):
        v = [V[c, at(x + 1)] for c in range(3)]
        dx_v = [(V[c, at(x + 2)] - V[c, at(x)]) * 0.5 for c in range(3)]
        dz_v = [dz(f, VZH[0, c, at(x)], VZH[1, c, at(x)]) for c, f in enumerate(v)]
        dy_v = [dy(f) for f in v]
        div = dx_v[0] + dz_v[1] + dy_v[2]
        third = div * (1.0 / 3.0)
        pres = pres - 0.25 * div
        PR[at(x)] = pres
        strain = (
            dx_v[0] - third,
            dz_v[1] - third,
            dy_v[2] - third,
            0.5 * (dx_v[1] + dz_v[0]),
            0.5 * (dx_v[2] + dy_v[0]),
            0.5 * (dz_v[2] + dy_v[1]),
        )
        twice = 2.0 * ETA[at(x)]
        trial = [
            twice * (strain[c] + OLD[c, at(x)] * (0.5 / shear_time_increment)) for c in range(6)
        ]
        tau_ii = jnp.sqrt(
            0.5 * (trial[0] * trial[0] + trial[1] * trial[1] + trial[2] * trial[2])
            + trial[3] * trial[3]
            + trial[4] * trial[4]
            + trial[5] * trial[5]
        )
        return pres, trial, tau_ii

    def first_trial(x, carry):
        _, trial, tau_ii = trial_stress(x, PIN[at(x)])
        for c in range(6):
            TAU[c, at(x)] = trial[c]
        TB[at(x)] = tau_ii
        return carry

    over_rows(first_trial)

    for pair in gz_copies:
        wait_got(pair)

    def smooth_z(x, carry):
        own, low, high = GX[at(x)], GZH[0, at(x)], GZH[1, at(x)]
        sum_ = gauss_weights[REACH] * own
        for k in range(1, REACH + 1):
            above = pltpu.roll(jnp.where(sub >= k, own, high), nz - k, 1)
            below = pltpu.roll(jnp.where(sub < nz - k, own, low), k, 1)
            sum_ = sum_ + gauss_weights[REACH + k] * (above + below)
        SM[at(x)] = sum_
        return carry

    over_rows(smooth_z)
    SM[...] = jnp.dot(
        SM[...].reshape(rows * nz, ny),
        YM[...],
        precision=lax.Precision.HIGHEST,
        preferred_element_type=jnp.float32,
    ).reshape(rows, nz, ny)

    half = ny // 2 if ny % 256 == 0 else ny
    tops = []
    for it in range(ITERS):
        last = it == ITERS - 1

        def stress_row(x, carry, it=it, last=last):
            most_f, most_eta = carry
            if it == 0:
                pres, trial, tau_ii = PR[at(x)], [TAU[c, at(x)] for c in range(6)], TB[at(x)]
                seeded = WK[at(x)].astype(jnp.float32)
                strength = 0.8660254 * ((1.0 - 0.6 * seeded) / (1.0 + 2.0 * SM[at(x)]))
                COH[at(x)] = strength
                plas = PLX[at(x + REACH)]
            else:
                pres, trial, tau_ii = trial_stress(x, PR[at(x)])
                strength = COH[at(x)]
                plas = PL[at(x)]
            eta = ETA[at(x)]
            yield_f = tau_ii - 0.5 * jnp.maximum(pres, 0.0) - strength
            dlam = jnp.maximum(yield_f, 0.0) / (eta + 0.5)
            shrink = 1.0 - eta * dlam / jnp.maximum(tau_ii, 0.5)
            tau = [shrink * value for value in trial]
            PL[at(x)] = plas + dlam
            if last:
                for c in range(6):
                    TAU[c, at(x)] = tau[c]
            SX[it, 0, at(x + 1)] = tau[0] - pres
            SX[it, 1, at(x + 1)] = tau[3]
            SX[it, 2, at(x + 1)] = tau[4]
            szz = tau[1] - pres
            TZ[0, at(x)] = szz
            TZ[1, at(x)] = tau[5]
            TZ[2, at(x)] = tau[2] - pres
            for c, f in enumerate((tau[3], szz, tau[5])):
                SZE[it, 0, c, at(x)] = f[:, 0:1]
                SZE[it, 1, c, at(x)] = f[:, nz - 1 : nz]
            return jnp.maximum(most_f, yield_f), jnp.maximum(most_eta, eta * shrink)

        start = jnp.full(many, -jnp.inf, jnp.float32)
        most_f, most_eta = over_rows(stress_row, (start, start))
        sx_copies = [
            exchange("xh", SX.at[it, :, pl.ds(rows, 1)], SX.at[it, :, pl.ds(0, 1)]),
            exchange("xl", SX.at[it, :, pl.ds(1, 1)], SX.at[it, :, pl.ds(rows + 1, 1)]),
        ]
        sz_copies = [
            exchange("zh", SZE.at[it, 1], SZH.at[it, 0]),
            exchange("zl", SZE.at[it, 0], SZH.at[it, 1]),
        ]

        def folded(most):
            most = jnp.max(jnp.max(most, axis=0), axis=0, keepdims=True)
            return jnp.maximum(most[:, :half], most[:, ny - half :])

        PK[it, me] = jnp.concatenate([folded(most_f), folded(most_eta)], axis=0)

        def tell(place, it=it):
            pltpu.make_async_remote_copy(
                src_ref=PK.at[it, me],
                dst_ref=PK.at[it, me],
                send_sem=pk_send.at[it],
                recv_sem=pk_recv.at[it],
                device_id=place,
                device_id_type=MESH,
            ).start()

        to_others(tell)
        for pair in sz_copies:
            wait_got(pair)

        def inner_row(x, carry, it=it):
            txz, txy = SX[it, 1, at(x + 1)], SX[it, 2, at(x + 1)]
            szz, tzy, syy = TZ[0, at(x)], TZ[1, at(x)], TZ[2, at(x)]
            z_terms = [
                dz(f, SZH[it, 0, c, at(x)], SZH[it, 1, c, at(x)])
                for c, f in enumerate((txz, szz, tzy))
            ]
            y_terms = [dy(f) for f in (txy, tzy, syy)]
            for c in range(3):
                R[c, at(x)] = z_terms[c] + y_terms[c]
            return carry

        def add_x(low, high, it=it):
            for c in range(3):
                R[c, low:high] = R[c, low:high] + 0.5 * (
                    SX[it, c, low + 2 : high + 2] - SX[it, c, low:high]
                )

        r_copies = []
        if not last:
            inner_row(0, 0)
            inner_row(rows - block, 0)
            for c in range(3):
                RP[0, c] = R[c, 0] + 0.5 * SX[it, c, 2]
                RP[1, c] = R[c, rows - 1] - 0.5 * SX[it, c, rows - 1]
            r_copies += [
                exchange("xh", RP.at[1], RH.at[0]),
                exchange("xl", RP.at[0], RH.at[1]),
            ]
        over_rows(inner_row)
        add_x(1, rows - 1)
        for pair in sx_copies:
            wait_got(pair)
        add_x(0, 1)
        add_x(rows - 1, rows)
        if not last:

            def edges(x, carry):
                for c in range(3):
                    value = R[c, at(x)]
                    RZE[0, c, at(x)] = value[:, 0:1]
                    RZE[1, c, at(x)] = value[:, nz - 1 : nz]
                return carry

            over_rows(edges)
            r_copies += [
                exchange("zh", RZE.at[1], RZH.at[0]),
                exchange("zl", RZE.at[0], RZH.at[1]),
            ]
            for pair in vel_copies:
                wait_sent(pair)
            for pair in r_copies:
                wait_got(pair)

        others = PK.at[it, pl.ds(0, total - 1)]
        arrived = pltpu.make_async_copy(others, others, pk_recv.at[it])
        arrived.wait()
        peaks = jnp.max(PK[it], axis=0)
        step = 0.125 / jnp.max(peaks[1:2], axis=1, keepdims=True)

        def velocity_row(x, carry):
            for c in range(3):
                value = V[c, at(x + 1)] + step * R[c, at(x)]
                if last:
                    VOUT[c, at(x)] = value
                else:
                    V[c, at(x + 1)] = value
            return carry

        over_rows(velocity_row)
        if not last:

            @pl.when(has["xl"])
            def _(it=it, step=step):
                for c in range(3):
                    V[c, 0] = V[c, 0] + step * (RH[0, c] + 0.5 * SX[it, c, 1])

            @pl.when(has["xh"])
            def _(it=it, step=step):
                for c in range(3):
                    V[c, rows + 1] = V[c, rows + 1] + step * (RH[1, c] - 0.5 * SX[it, c, rows])

            VZH[...] = VZH[...] + step * RZH[...]
        tops.append(jnp.max(peaks[0:1], axis=1, keepdims=True))
        for pair in sx_copies + sz_copies + r_copies:
            wait_sent(pair)
        pltpu.make_async_copy(others, others, pk_send.at[it]).wait()

    peak_out[...] = jnp.concatenate(tops, axis=1)[0]
    for pair in plas_copies + vz_copies + gz_copies:
        wait_sent(pair)


def store_kernel(*refs):
    held, out, sem = refs[:5], refs[5:10], refs[10]
    copies = [pltpu.make_async_copy(a, b, sem.at[i]) for i, (a, b) in enumerate(zip(held, out))]
    for copy in copies:
        copy.start()
    for copy in copies:
        copy.wait()


def solution(mesh):
    gx_count, gz_count = mesh.shape["gx"], mesh.shape["gz"]
    total = gx_count * gz_count

    def per_device(velocity, pressure, stress_old, plastic, viscosity, weak_seed):
        rows, nz, ny = pressure.shape
        cells = (rows, nz, ny)
        f32 = jnp.float32
        vm = lambda *shape: pltpu.VMEM(shape, f32)
        copies = 6 + 2 + 4 * ITERS + 4 * (ITERS - 1)
        anywhere = pl.BlockSpec(memory_space=pl.ANY)
        shapes = (velocity.shape, pressure.shape, stress_old.shape, plastic.shape)
        held = pl.pallas_call(
            functools.partial(kernel, gx_count, gz_count),
            out_shape=tuple(vm(*shape) for shape in shapes + ((ITERS,),)),
            in_specs=[anywhere] * 6,
            out_specs=(pl.BlockSpec(memory_space=pltpu.VMEM),) * 5,
            scratch_shapes=[
                vm(3, rows + 2, nz, ny),
                vm(*cells),
                vm(6, *cells),
                vm(rows + 2 * REACH, nz, ny),
                vm(*cells),
                pltpu.VMEM(cells, jnp.int32),
                vm(*cells),
                vm(*cells),
                vm(ny, ny),
                vm(*cells),
                vm(2, *cells),
                vm(*cells),
                vm(2, 3, rows, 1, ny),
                vm(2, 3, rows, 1, ny),
                vm(ITERS, 3, rows + 2, nz, ny),
                vm(3, *cells),
                vm(ITERS, 2, 3, rows, 1, ny),
                vm(ITERS, 2, 3, rows, 1, ny),
                vm(2, 3, nz, ny),
                vm(2, 3, nz, ny),
                vm(3, *cells),
                vm(2, 3, rows, 1, ny),
                vm(2, 3, rows, 1, ny),
                vm(*cells),
                vm(ITERS, total, 2, ny // 2 if ny % 256 == 0 else ny),
                pltpu.SemaphoreType.DMA((6,)),
                pltpu.SemaphoreType.DMA((copies,)),
                pltpu.SemaphoreType.DMA((copies,)),
                pltpu.SemaphoreType.DMA((ITERS,)),
                pltpu.SemaphoreType.DMA((ITERS,)),
            ],
            compiler_params=pltpu.CompilerParams(collective_id=0, has_side_effects=True),
        )(velocity, pressure, stress_old, plastic, viscosity, weak_seed)
        held = [pltpu.with_memory_space_constraint(array, pltpu.VMEM) for array in held]
        return pl.pallas_call(
            store_kernel,
            out_shape=tuple(jax.ShapeDtypeStruct(shape, f32) for shape in shapes)
            + (jax.ShapeDtypeStruct((ITERS,), f32),),
            in_specs=[anywhere] * 5,
            out_specs=(anywhere,) * 5,
            scratch_shapes=[pltpu.SemaphoreType.DMA((5,))],
        )(*held)

    in_specs = (
        P(None, "gx", "gz", None),
        P("gx", "gz", None),
        P(None, "gx", "gz", None),
        P("gx", "gz", None),
        P("gx", "gz", None),
        P("gx", "gz", None),
    )
    out_specs = (
        P(None, "gx", "gz", None),
        P("gx", "gz", None),
        P(None, "gx", "gz", None),
        P("gx", "gz", None),
        P(),
    )
    return jax.shard_map(
        per_device, mesh=mesh, in_specs=in_specs, out_specs=out_specs, check_vma=False
    )
```
